32 devices in a mesh: row: 8 (over z, y), kk: 4 (over x, core).
Axes of the slice: x: 2, y: 2, z: 4, core: 2. Of those that a mesh axis runs over, the one named last changes fastest.
Arguments:
- left_blocks: bfloat16 [4096, 4096], P('row', 'kk'), may hold values from -6 to 6
- right_blocks: bfloat16 [4096, 1024], P('kk', 'row'), may hold values from -0.125 to 0.125
- left_mask: int32 [32, 32], P('row', 'kk'), may hold values 0 or 1
- right_mask: int32 [32, 8], P('kk', 'row'), may hold values 0 or 1
- out_mask: int32 [32, 8], P('row'), may hold values 0 or 1
Outputs:
- product_blocks: bfloat16 [4096, 1024], P(('row', 'kk'))
The draws below stay inside these ranges and needn't reach their ends.
All inputs are finite; a program needn't handle non-finite values. No bound on the sum of `left_mask` or of `right_mask` or of `out_mask` on one device may be relied on, other than what follows from the above.
Results may differ from the reference program's by a relative error of at most 0.001.
Values may be sent and summed in bfloat16 or wider, within the bound.
A program may use at most 192 MiB of HBM per device.

```python
import jax
import jax.numpy as jnp

BS = 128
KB = 32
IB = 32
JB = 8


def with_ends(values, key, least, top_value):
    shape = values.shape
    spot = [jax.random.randint(jax.random.fold_in(key, axis), (), 0, shape[axis]) for axis in range(len(shape))]
    values = values.at[tuple(spot)].set(least)
    longest = shape.index(max(shape))
    spot[longest] = (spot[longest] + 1) % shape[longest]
    return values.at[tuple(spot)].set(top_value)


def steps_of(rng, extent, split, least, high):
    gain = 1.0
    for axis_at, shards_of in split:
        draws = jax.random.uniform(jax.random.fold_in(jax.random.fold_in(rng, 6), axis_at), (shards_of,), jnp.float32, least / len(split), high / len(split))
        gain = gain * jnp.repeat(jnp.exp(draws), extent[axis_at] // shards_of).reshape((-1,) + (1,) * (len(extent) - 1 - axis_at))
    return gain


def normal_values(stream_key, dims, deviation, most, split=(), kind=jnp.bfloat16):
    entries = jax.random.normal(stream_key, dims, jnp.float32) * deviation
    if len(split) > 0:
        entries = steps_of(stream_key, dims, split, -0.22, 0.18) * entries
    return jnp.clip(entries, min=-most, max=most).astype(kind)


def setup_inputs(seed: int = 0) -> dict:
    key_list = jax.random.split(jax.random.key(seed), 6)
    return {
        "left_blocks": normal_values(key_list[0], (IB * BS, KB * BS), 1.0, 6.0, ((0, 8), (1, 4))),
        "right_blocks": normal_values(key_list[1], (KB * BS, JB * BS), (KB * BS // 2) ** -0.5, 0.125, ((0, 4), (1, 8))),
        "left_mask": with_ends((jax.random.randint(key_list[2], (IB, KB), 0, 2) < 1).astype(jnp.int32), jax.random.fold_in(key_list[2], 1), 0, 1),
        "right_mask": with_ends((jax.random.randint(key_list[3], (KB, JB), 0, 2) < 1).astype(jnp.int32), jax.random.fold_in(key_list[3], 1), 0, 1),
        "out_mask": with_ends((jax.random.randint(key_list[4], (IB, JB), 0, 4) < 3).astype(jnp.int32), jax.random.fold_in(key_list[4], 1), 0, 1),
    }


def expand(mask, size):
    return jnp.repeat(jnp.repeat(mask, size, axis=0), size, axis=1)


def reference(left_blocks, right_blocks, left_mask, right_mask, out_mask):
    left_used = left_blocks * expand(left_mask, BS).astype(jnp.bfloat16)
    right_used = right_blocks * expand(right_mask, BS).astype(jnp.bfloat16)
    full = jnp.dot(left_used, right_used, preferred_element_type=jnp.float32)
    return (full * expand(out_mask, BS).astype(jnp.float32)).astype(jnp.bfloat16)
```

```python
import functools

import jax
import jax.numpy as jnp
from jax import lax
from jax.experimental import pallas as pl
from jax.experimental.pallas import tpu as pltpu
from jax.sharding import PartitionSpec as P

MESH = pl.DeviceIdType.MESH
PIECES = 4


def kernel(
    rows_n,
    kk_n,
    left_hbm,
    right_hbm,
    left_mask,
    right_mask,
    out_mask,
    out_ref,
    left_raw,
    right_raw,
    left,
    right_all,
    s1_out,
    s1_in,
    keep,
    s2_in,
    load_sem,
    recv_sem,
    line_sem,
    mate_sem,
    s1_send,
    s1_recv,
    s2_send,
    s2_recv,
):
    depth, cols = right_raw.shape
    share = out_ref.shape[0]
    block = left_raw.shape[0] // left_mask.shape[0]
    kblocks = left_mask.shape[1]
    outer = rows_n // 2
    peers = kk_n // 2
    piece = depth // PIECES

    row = lax.axis_index("row")
    kk = lax.axis_index("kk")
    o, i = row // 2, row % 2
    b, c = kk // 2, kk % 2
    has_up, has_down = o + 1 < outer, o >= 1
    mate = {"row": o * 2 + 1 - i}
    up, down = {"row": row + 2}, {"row": row - 2}
    partner = {"kk": b * 2 + 1 - c}

    def peer(j):
        return lax.rem(b + j, peers)

    load_right = pltpu.make_async_copy(right_hbm, right_raw, load_sem.at[0])
    load_left = pltpu.make_async_copy(left_hbm, left_raw, load_sem.at[1])
    load_right.start()
    load_left.start()

    barrier = pltpu.get_barrier_semaphore()

    def greet(device):
        pl.semaphore_signal(barrier, inc=1, device_id=device, device_id_type=MESH)

    greet(mate)
    greet(partner)
    for j in range(1, peers):
        greet({"kk": peer(j) * 2 + c})

    @pl.when(has_up)
    def _():
        greet(up)

    @pl.when(has_down)
    def _():
        greet(down)

    load_right.wait()
    for kb in range(kblocks):
        part = pl.ds(kb * block, block)
        scale = right_mask[kb, 0].astype(jnp.float32)
        right_all[row, part, :] = (right_raw[part, :].astype(jnp.float32) * scale).astype(jnp.bfloat16)

    pl.semaphore_wait(barrier, 1 + peers + has_up.astype(jnp.int32) + has_down.astype(jnp.int32))

    def gather_copy(slot, p, sem, device):
        ref = right_all.at[slot, pl.ds(p * piece, piece), :]
        return pltpu.make_async_remote_copy(
            src_ref=ref, dst_ref=ref, send_sem=sem, recv_sem=recv_sem.at[slot, p], device_id=device, device_id_type=MESH
        )

    def up_copy(slot, p):
        return gather_copy(slot, p, line_sem.at[slot, p], up)

    def down_copy(slot, p, at=None):
        return gather_copy(slot, p, line_sem.at[slot if at is None else at, p], down)

    def mate_copy(slot, p):
        return gather_copy(slot, p, mate_sem.at[slot, p], mate)

    def s1_copy(slot):
        return pltpu.make_async_remote_copy(
            src_ref=s1_out.at[slot], dst_ref=s1_in.at[slot], send_sem=s1_send.at[slot], recv_sem=s1_recv.at[slot],
            device_id=partner, device_id_type=MESH,
        )

    def s2_copy(slot, j):
        to = peer(j)
        return pltpu.make_async_remote_copy(
            src_ref=keep.at[slot, to], dst_ref=s2_in.at[slot, j - 1], send_sem=s2_send.at[slot, j - 1],
            recv_sem=s2_recv.at[slot, j - 1], device_id={"kk": to * 2 + c}, device_id_type=MESH,
        )

    def process(slot):
        block_in = right_all[slot]
        half = peers * share
        s1_out[slot] = jnp.dot(left[0:half, :], block_in, preferred_element_type=jnp.float32)
        s1_copy(slot).start()
        got = jnp.dot(left[half : 2 * half, :], block_in, preferred_element_type=jnp.float32)
        for t in range(peers):
            keep[slot, t] = got[t * share : (t + 1) * share]

    def combine1(slot):
        s1_copy(slot).wait_recv()
        for t in range(peers):
            keep[slot, t] = keep[slot, t] + s1_in[slot, t * share : (t + 1) * share]
        for j in range(1, peers):
            s2_copy(slot, j).start()

    def combine2(slot):
        total = keep[slot, b]
        for j in range(1, peers):
            s2_copy(slot, j).wait_recv()
            total = total + s2_in[slot, j - 1]
        per = cols // block
        own = kk * share // block
        at = pl.multiple_of(slot * cols, cols)
        scale = out_mask[own, slot * per].astype(jnp.float32)
        out_ref[:, pl.ds(at, cols)] = (total * scale).astype(jnp.bfloat16)

    def ordered(n):
        low = jnp.minimum(o, outer - 1 - o)
        near = (n + 1) // 2
        paired = o + jnp.where(n % 2 == 1, -near, near)
        far = n - low
        single = o + jnp.where(o < outer - 1 - o, far, -far)
        return jnp.where(n <= 2 * low, paired, single)

    def mate_slot(n):
        return ordered(n) * 2 + 1 - i

    for p in range(PIECES):
        mate_copy(row, p).start()

        @pl.when(has_up)
        def _():
            up_copy(row, p).start()

        @pl.when(has_down)
        def _():
            down_copy(row, p, rows_n).start()

    load_left.wait()
    for s in range(2):
        for t in range(peers):
            src = pl.multiple_of((2 * t + (1 - c if s == 0 else c)) * share, share)
            dst = (s * peers + t) * share
            for q in range(share // block):
                for kb in range(kblocks):
                    scale = left_mask[src // block + q, kb].astype(jnp.float32)
                    lanes = pl.ds(kb * block, block)
                    tile = left_raw[pl.ds(pl.multiple_of(src + q * block, block), block), lanes]
                    left[dst + q * block : dst + (q + 1) * block, kb * block : (kb + 1) * block] = (
                        tile.astype(jnp.float32) * scale
                    ).astype(jnp.bfloat16)

    process(row)
    combine1(row)

    def at_distance(d, low_fn, high_fn):
        @pl.when(o - d >= 0)
        def _():
            low_fn(row - 2 * d)

        @pl.when((o + d < outer) & (d >= 1))
        def _():
            high_fn(row + 2 * d)

    def both(d, fn):
        at_distance(d, fn, fn)

    def tick(d, carry):
        for p in range(PIECES):

            def from_low(slot):
                mate_copy(slot, p).wait_recv()

                @pl.when(has_up)
                def _():
                    up_copy(slot, p).start()

                mate_copy(slot, p).start()

            def from_high(slot):
                mate_copy(slot, p).wait_recv()

                @pl.when(has_down)
                def _():
                    down_copy(slot, p).start()

                mate_copy(slot, p).start()

            at_distance(d, from_low, from_high)
        both(d, process)
        mslot = mate_slot(d - 1)
        for p in range(PIECES):
            mate_copy(mslot, p).wait_recv()
        process(mslot)
        both(d, combine1)
        combine1(mslot)
        both(d - 1, combine2)

        @pl.when(d >= 2)
        def _():
            combine2(mate_slot(d - 2))

        return carry

    lax.fori_loop(1, outer, tick, 0)

    last = mate_slot(outer - 1)
    for p in range(PIECES):
        mate_copy(last, p).wait_recv()
    process(last)
    both(outer - 1, combine2)
    if outer >= 2:
        combine2(mate_slot(outer - 2))
    combine1(last)
    combine2(last)

    def drain(slot, carry):
        s1_copy(slot).wait_send()
        for j in range(1, peers):
            s2_copy(slot, j).wait_send()
        so = slot // 2

        @pl.when(slot % 2 == i)
        def _():
            for p in range(PIECES):
                mate_copy(slot, p).wait_send()

                @pl.when(has_up & (so <= o))
                def _():
                    up_copy(slot, p).wait_send()

                @pl.when(has_down & (so > o))
                def _():
                    down_copy(slot, p).wait_send()

        return carry

    lax.fori_loop(0, rows_n, drain, 0)

    @pl.when(has_down)
    def _():
        for p in range(PIECES):
            down_copy(row, p, rows_n).wait_send()


def per_device(rows_n, kk_n, left_blocks, right_blocks, left_mask, right_mask, out_mask):
    rows = left_blocks.shape[0]
    depth, cols = right_blocks.shape
    share = rows // kk_n
    peers = kk_n // 2
    half = peers * share
    dma = pltpu.SemaphoreType.DMA
    f32, bf16 = jnp.float32, jnp.bfloat16
    return pl.pallas_call(
        functools.partial(kernel, rows_n, kk_n),
        out_shape=jax.ShapeDtypeStruct((share, rows_n * cols), bf16),
        in_specs=[pl.BlockSpec(memory_space=pl.ANY)] * 2 + [pl.BlockSpec(memory_space=pltpu.SMEM)] * 3,
        out_specs=pl.BlockSpec(memory_space=pltpu.VMEM),
        scratch_shapes=[
            pltpu.VMEM((rows, depth), bf16),
            pltpu.VMEM((depth, cols), bf16),
            pltpu.VMEM((rows, depth), bf16),
            pltpu.VMEM((rows_n, depth, cols), bf16),
            pltpu.VMEM((rows_n, half, cols), f32),
            pltpu.VMEM((rows_n, half, cols), f32),
            pltpu.VMEM((rows_n, peers, share, cols), f32),
            pltpu.VMEM((rows_n, max(peers - 1, 1), share, cols), f32),
            dma((2,)),
            dma((rows_n, PIECES)),
            dma((rows_n + 1, PIECES)),
            dma((rows_n, PIECES)),
            dma((rows_n,)),
            dma((rows_n,)),
            dma((rows_n, max(peers - 1, 1))),
            dma((rows_n, max(peers - 1, 1))),
        ],
        compiler_params=pltpu.CompilerParams(
            collective_id=0, has_side_effects=True, vmem_limit_bytes=62 * 1024 * 1024
        ),
    )(left_blocks, right_blocks, left_mask, right_mask, out_mask)


def solution(mesh):
    in_specs = (P("row", "kk"), P("kk", "row"), P("row", "kk"), P("kk", "row"), P("row", None))
    out_specs = P(("row", "kk"), None)
    body = functools.partial(per_device, mesh.shape["row"], mesh.shape["kk"])
    return jax.shard_map(body, mesh=mesh, in_specs=in_specs, out_specs=out_specs, check_vma=False)
```

```python
import functools

import jax
import jax.numpy as jnp
from jax import lax
from jax.experimental import pallas as pl
from jax.experimental.pallas import tpu as pltpu
from jax.sharding import PartitionSpec as P

MESH = pl.DeviceIdType.MESH
PIECES = 2


def kernel(
    rows_n,
    kk_n,
    left_hbm,
    right_hbm,
    left_mask,
    right_mask,
    out_mask,
    out_ref,
    left_raw,
    right_raw,
    left,
    right_all,
    s1_out,
    s1_in,
    keep,
    s2_in,
    load_sem,
    recv_sem,
    line_sem,
    mate_sem,
    s1_send,
    s1_recv,
    s2_send,
    s2_recv,
):
    depth, cols = right_raw.shape
    share = out_ref.shape[0]
    block = left_raw.shape[0] // left_mask.shape[0]
    kblocks = left_mask.shape[1]
    outer = rows_n // 2
    peers = kk_n // 2
    piece = depth // PIECES

    row = lax.axis_index("row")
    kk = lax.axis_index("kk")
    o, i = row // 2, row % 2
    b, c = kk // 2, kk % 2
    has_up, has_down = o + 1 < outer, o >= 1
    mate = {"row": o * 2 + 1 - i}
    up, down = {"row": row + 2}, {"row": row - 2}
    partner = {"kk": b * 2 + 1 - c}

    def peer(j):
        return lax.rem(b + j, peers)

    load_right = pltpu.make_async_copy(right_hbm, right_raw, load_sem.at[0])
    load_left = pltpu.make_async_copy(left_hbm, left_raw, load_sem.at[1])
    load_right.start()
    load_left.start()

    barrier = pltpu.get_barrier_semaphore()

    def greet(device):
        pl.semaphore_signal(barrier, inc=1, device_id=device, device_id_type=MESH)

    greet(mate)
    greet(partner)
    for j in range(1, peers):
        greet({"kk": peer(j) * 2 + c})

    @pl.when(has_up)
    def _():
        greet(up)

    @pl.when(has_down)
    def _():
        greet(down)

    load_right.wait()
    for kb in range(kblocks):
        part = pl.ds(kb * block, block)
        scale = right_mask[kb].astype(jnp.float32)
        right_all[row, part, :] = (right_raw[part, :].astype(jnp.float32) * scale).astype(jnp.bfloat16)

    pl.semaphore_wait(barrier, 1 + peers + has_up.astype(jnp.int32) + has_down.astype(jnp.int32))

    def gather_copy(slot, p, sem, device):
        ref = right_all.at[slot, pl.ds(p * piece, piece), :]
        return pltpu.make_async_remote_copy(
            src_ref=ref, dst_ref=ref, send_sem=sem, recv_sem=recv_sem.at[slot, p], device_id=device, device_id_type=MESH
        )

    def up_copy(slot, p):
        return gather_copy(slot, p, line_sem.at[slot, p], up)

    def down_copy(slot, p, at=None):
        return gather_copy(slot, p, line_sem.at[slot if at is None else at, p], down)

    def mate_copy(slot, p):
        return gather_copy(slot, p, mate_sem.at[slot, p], mate)

    def s1_copy(slot):
        return pltpu.make_async_remote_copy(
            src_ref=s1_out.at[slot], dst_ref=s1_in.at[slot], send_sem=s1_send.at[slot], recv_sem=s1_recv.at[slot],
            device_id=partner, device_id_type=MESH,
        )

    def s2_copy(slot, j):
        to = peer(j)
        return pltpu.make_async_remote_copy(
            src_ref=keep.at[slot, to], dst_ref=s2_in.at[slot, j - 1], send_sem=s2_send.at[slot, j - 1],
            recv_sem=s2_recv.at[slot, j - 1], device_id={"kk": to * 2 + c}, device_id_type=MESH,
        )

    def process(slot):
        block_in = right_all[slot]
        half = peers * share
        s1_out[slot] = jnp.dot(left[0:half, :], block_in, preferred_element_type=jnp.float32)
        s1_copy(slot).start()
        got = jnp.dot(left[half : 2 * half, :], block_in, preferred_element_type=jnp.float32)
        for t in range(peers):
            keep[slot, t] = got[t * share : (t + 1) * share]

    def combine1(slot):
        s1_copy(slot).wait_recv()
        for t in range(peers):
            keep[slot, t] = keep[slot, t] + s1_in[slot, t * share : (t + 1) * share]
        for j in range(1, peers):
            s2_copy(slot, j).start()

    def combine2(slot):
        total = keep[slot, b]
        for j in range(1, peers):
            s2_copy(slot, j).wait_recv()
            total = total + s2_in[slot, j - 1]
        per = cols // block
        own = kk * share // block
        at = pl.multiple_of(slot * cols, cols)
        scale = out_mask[own, slot * per].astype(jnp.float32)
        out_ref[:, pl.ds(at, cols)] = (total * scale).astype(jnp.bfloat16)

    def ordered(n):
        low = jnp.minimum(o, outer - 1 - o)
        near = (n + 1) // 2
        paired = o + jnp.where(n % 2 == 1, -near, near)
        far = n - low
        single = o + jnp.where(o < outer - 1 - o, far, -far)
        return jnp.where(n <= 2 * low, paired, single)

    def mate_slot(n):
        return ordered(n) * 2 + 1 - i

    for p in range(PIECES):
        mate_copy(row, p).start()

        @pl.when(has_up)
        def _():
            up_copy(row, p).start()

        @pl.when(has_down)
        def _():
            down_copy(row, p, rows_n).start()

    load_left.wait()
    for s in range(2):
        for t in range(peers):
            src = pl.multiple_of((2 * t + (1 - c if s == 0 else c)) * share, share)
            dst = (s * peers + t) * share
            for q in range(share // block):
                for kb in range(kblocks):
                    scale = left_mask[src // block + q, kb].astype(jnp.float32)
                    lanes = pl.ds(kb * block, block)
                    tile = left_raw[pl.ds(pl.multiple_of(src + q * block, block), block), lanes]
                    left[dst + q * block : dst + (q + 1) * block, kb * block : (kb + 1) * block] = (
                        tile.astype(jnp.float32) * scale
                    ).astype(jnp.bfloat16)

    process(row)
    combine1(row)

    def at_distance(d, low_fn, high_fn):
        @pl.when(o - d >= 0)
        def _():
            low_fn(row - 2 * d)

        @pl.when((o + d < outer) & (d >= 1))
        def _():
            high_fn(row + 2 * d)

    def both(d, fn):
        at_distance(d, fn, fn)

    def tick(d, carry):
        for p in range(PIECES):

            def from_low(slot):
                mate_copy(slot, p).wait_recv()

                @pl.when(has_up)
                def _():
                    up_copy(slot, p).start()

                mate_copy(slot, p).start()

            def from_high(slot):
                mate_copy(slot, p).wait_recv()

                @pl.when(has_down)
                def _():
                    down_copy(slot, p).start()

                mate_copy(slot, p).start()

            at_distance(d, from_low, from_high)
        both(d, process)
        mslot = mate_slot(d - 1)
        for p in range(PIECES):
            mate_copy(mslot, p).wait_recv()
        process(mslot)
        both(d, combine1)
        combine1(mslot)
        both(d - 1, combine2)

        @pl.when(d >= 2)
        def _():
            combine2(mate_slot(d - 2))

        return carry

    lax.fori_loop(1, outer, tick, 0)

    last = mate_slot(outer - 1)
    for p in range(PIECES):
        mate_copy(last, p).wait_recv()
    process(last)
    combine1(last)
    both(outer - 1, combine2)
    if outer >= 2:
        combine2(mate_slot(outer - 2))
    combine2(last)

    def drain(slot, carry):
        s1_copy(slot).wait_send()
        for j in range(1, peers):
            s2_copy(slot, j).wait_send()
        so = slot // 2

        @pl.when(slot % 2 == i)
        def _():
            for p in range(PIECES):
                mate_copy(slot, p).wait_send()

                @pl.when(has_up & (so <= o))
                def _():
                    up_copy(slot, p).wait_send()

                @pl.when(has_down & (so > o))
                def _():
                    down_copy(slot, p).wait_send()

        return carry

    lax.fori_loop(0, rows_n, drain, 0)

    @pl.when(has_down)
    def _():
        for p in range(PIECES):
            down_copy(row, p, rows_n).wait_send()


def per_device(rows_n, kk_n, left_blocks, right_blocks, left_mask, right_mask, out_mask):
    rows = left_blocks.shape[0]
    depth, cols = right_blocks.shape
    share = rows // kk_n
    peers = kk_n // 2
    half = peers * share
    dma = pltpu.SemaphoreType.DMA
    f32, bf16 = jnp.float32, jnp.bfloat16
    return pl.pallas_call(
        functools.partial(kernel, rows_n, kk_n),
        out_shape=jax.ShapeDtypeStruct((share, rows_n * cols), bf16),
        in_specs=[pl.BlockSpec(memory_space=pl.ANY)] * 2 + [pl.BlockSpec(memory_space=pltpu.SMEM)] * 3,
        out_specs=pl.BlockSpec(memory_space=pltpu.VMEM),
        scratch_shapes=[
            pltpu.VMEM((rows, depth), bf16),
            pltpu.VMEM((depth, cols), bf16),
            pltpu.VMEM((rows, depth), bf16),
            pltpu.VMEM((rows_n, depth, cols), bf16),
            pltpu.VMEM((rows_n, half, cols), f32),
            pltpu.VMEM((rows_n, half, cols), f32),
            pltpu.VMEM((rows_n, peers, share, cols), f32),
            pltpu.VMEM((rows_n, max(peers - 1, 1), share, cols), f32),
            dma((2,)),
            dma((rows_n, PIECES)),
            dma((rows_n + 1, PIECES)),
            dma((rows_n, PIECES)),
            dma((rows_n,)),
            dma((rows_n,)),
            dma((rows_n, max(peers - 1, 1))),
            dma((rows_n, max(peers - 1, 1))),
        ],
        compiler_params=pltpu.CompilerParams(
            collective_id=0, has_side_effects=True, vmem_limit_bytes=62 * 1024 * 1024
        ),
    )(left_blocks, right_blocks, left_mask, right_mask.reshape(-1), out_mask)


def solution(mesh):
    in_specs = (P("row", "kk"), P("kk", "row"), P("row", "kk"), P("kk", "row"), P("row", None))
    out_specs = P(("row", "kk"), None)
    body = functools.partial(per_device, mesh.shape["row"], mesh.shape["kk"])
    return jax.shard_map(body, mesh=mesh, in_specs=in_specs, out_specs=out_specs, check_vma=False)
```

```python
import functools

import jax
import jax.numpy as jnp
from jax import lax
from jax.experimental import pallas as pl
from jax.experimental.pallas import tpu as pltpu
from jax.sharding import PartitionSpec as P

MESH = pl.DeviceIdType.MESH
PIECES = 2
VMEM_BYTES = 67043328
SPARE = 256 * 1024


def kernel(
    rows_n,
    kk_n,
    left_hbm,
    right_hbm,
    left_mask,
    right_mask,
    out_mask,
    out_ref,
    left_raw,
    right_raw,
    left,
    right_all,
    s1_out,
    s1_in,
    keep,
    s2_in,
    load_sem,
    recv_sem,
    line_sem,
    mate_sem,
    s1_send,
    s1_recv,
    s2_send,
    s2_recv,
):
    depth, cols = right_raw.shape
    share = out_ref.shape[0]
    block = left_raw.shape[0] // left_mask.shape[0]
    kblocks = left_mask.shape[1]
    outer = rows_n // 2
    peers = kk_n // 2
    piece = depth // PIECES

    row = lax.axis_index("row")
    kk = lax.axis_index("kk")
    o, i = row // 2, row % 2
    b, c = kk // 2, kk % 2
    has_up, has_down = o + 1 < outer, o >= 1
    mate = {"row": o * 2 + 1 - i}
    up, down = {"row": row + 2}, {"row": row - 2}
    partner = {"kk": b * 2 + 1 - c}

    def peer(j):
        return lax.rem(b + j, peers)

    load_right = pltpu.make_async_copy(right_hbm, right_raw, load_sem.at[0])
    load_left = pltpu.make_async_copy(left_hbm, left_raw, load_sem.at[1])
    load_right.start()
    load_left.start()

    barrier = pltpu.get_barrier_semaphore()

    def greet(device):
        pl.semaphore_signal(barrier, inc=1, device_id=device, device_id_type=MESH)

    greet(mate)
    greet(partner)
    for j in range(1, peers):
        greet({"kk": peer(j) * 2 + c})

    @pl.when(has_up)
    def _():
        greet(up)

    @pl.when(has_down)
    def _():
        greet(down)

    load_right.wait()
    for kb in range(kblocks):
        part = pl.ds(kb * block, block)
        scale = right_mask[kb].astype(jnp.float32)
        right_all[row, part, :] = (right_raw[part, :].astype(jnp.float32) * scale).astype(jnp.bfloat16)

    pl.semaphore_wait(barrier, 1 + peers + has_up.astype(jnp.int32) + has_down.astype(jnp.int32))

    def gather_copy(slot, p, sem, device):
        first = depth * 3 // 8
        ref = right_all.at[slot, pl.ds(p * first, first if p == 0 else depth - first), :]
        return pltpu.make_async_remote_copy(
            src_ref=ref, dst_ref=ref, send_sem=sem, recv_sem=recv_sem.at[slot, p], device_id=device, device_id_type=MESH
        )

    def up_copy(slot, p):
        return gather_copy(slot, p, line_sem.at[slot, p], up)

    def down_copy(slot, p, at=None):
        return gather_copy(slot, p, line_sem.at[slot if at is None else at, p], down)

    def mate_copy(slot, p):
        return gather_copy(slot, p, mate_sem.at[slot, p], mate)

    def s1_copy(slot):
        return pltpu.make_async_remote_copy(
            src_ref=s1_out.at[slot], dst_ref=s1_in.at[slot], send_sem=s1_send.at[slot], recv_sem=s1_recv.at[slot],
            device_id=partner, device_id_type=MESH,
        )

    def s2_copy(slot, j):
        to = peer(j)
        return pltpu.make_async_remote_copy(
            src_ref=keep.at[slot, to], dst_ref=s2_in.at[slot, j - 1], send_sem=s2_send.at[slot, j - 1],
            recv_sem=s2_recv.at[slot, j - 1], device_id={"kk": to * 2 + c}, device_id_type=MESH,
        )

    def process(slot):
        block_in = right_all[slot]
        half = peers * share
        s1_out[slot] = jnp.dot(left[0:half, :], block_in, preferred_element_type=jnp.float32)
        s1_copy(slot).start()
        got = jnp.dot(left[half : 2 * half, :], block_in, preferred_element_type=jnp.float32)
        for t in range(peers):
            keep[slot, t] = got[t * share : (t + 1) * share]

    def combine1(slot):
        s1_copy(slot).wait_recv()
        for t in range(peers):
            keep[slot, t] = keep[slot, t] + s1_in[slot, t * share : (t + 1) * share]
        for j in range(1, peers):
            s2_copy(slot, j).start()

    def combine2(slot):
        total = keep[slot, b]
        for j in range(1, peers):
            s2_copy(slot, j).wait_recv()
            total = total + s2_in[slot, j - 1]
        per = cols // block
        own = kk * share // block
        at = pl.multiple_of(slot * cols, cols)
        scale = out_mask[own, slot * per].astype(jnp.float32)
        out_ref[:, pl.ds(at, cols)] = (total * scale).astype(jnp.bfloat16)

    def ordered(n):
        low = jnp.minimum(o, outer - 1 - o)
        near = (n + 1) // 2
        paired = o + jnp.where(n % 2 == 1, -near, near)
        far = n - low
        single = o + jnp.where(o < outer - 1 - o, far, -far)
        return jnp.where(n <= 2 * low, paired, single)

    def mate_slot(n):
        return ordered(n) * 2 + 1 - i

    for p in range(PIECES):
        mate_copy(row, p).start()

        @pl.when(has_up)
        def _():
            up_copy(row, p).start()

        @pl.when(has_down)
        def _():
            down_copy(row, p, rows_n).start()

    load_left.wait()
    for s in range(2):
        for t in range(peers):
            src = pl.multiple_of((2 * t + (1 - c if s == 0 else c)) * share, share)
            dst = (s * peers + t) * share
            for q in range(share // block):
                for kb in range(kblocks):
                    scale = left_mask[src // block + q, kb].astype(jnp.float32)
                    lanes = pl.ds(kb * block, block)
                    tile = left_raw[pl.ds(pl.multiple_of(src + q * block, block), block), lanes]
                    left[dst + q * block : dst + (q + 1) * block, kb * block : (kb + 1) * block] = (
                        tile.astype(jnp.float32) * scale
                    ).astype(jnp.bfloat16)

    process(row)
    combine1(row)

    def at_distance(d, low_fn, high_fn):
        @pl.when(o - d >= 0)
        def _():
            low_fn(row - 2 * d)

        @pl.when((o + d < outer) & (d >= 1))
        def _():
            high_fn(row + 2 * d)

    def both(d, fn):
        at_distance(d, fn, fn)

    def tick(d, carry):
        for p in range(PIECES):

            def from_low(slot):
                mate_copy(slot, p).wait_recv()

                @pl.when(has_up)
                def _():
                    up_copy(slot, p).start()

                mate_copy(slot, p).start()

            def from_high(slot):
                mate_copy(slot, p).wait_recv()

                @pl.when(has_down)
                def _():
                    down_copy(slot, p).start()

                mate_copy(slot, p).start()

            at_distance(d, from_low, from_high)
        both(d, process)
        mslot = mate_slot(d - 1)
        for p in range(PIECES):
            mate_copy(mslot, p).wait_recv()
        process(mslot)
        both(d, combine1)
        combine1(mslot)
        both(d - 1, combine2)

        @pl.when(d >= 2)
        def _():
            combine2(mate_slot(d - 2))

        return carry

    lax.fori_loop(1, outer, tick, 0)

    last = mate_slot(outer - 1)
    for p in range(PIECES):
        mate_copy(last, p).wait_recv()
    process(last)
    combine1(last)
    both(outer - 1, combine2)
    if outer >= 2:
        combine2(mate_slot(outer - 2))
    combine2(last)

    def drain(slot, carry):
        s1_copy(slot).wait_send()
        for j in range(1, peers):
            s2_copy(slot, j).wait_send()
        so = slot // 2

        @pl.when(slot % 2 == i)
        def _():
            for p in range(PIECES):
                mate_copy(slot, p).wait_send()

                @pl.when(has_up & (so <= o))
                def _():
                    up_copy(slot, p).wait_send()

                @pl.when(has_down & (so > o))
                def _():
                    down_copy(slot, p).wait_send()

        return carry

    lax.fori_loop(0, rows_n, drain, 0)

    @pl.when(has_down)
    def _():
        for p in range(PIECES):
            down_copy(row, p, rows_n).wait_send()


def per_device(rows_n, kk_n, left_blocks, right_blocks, left_mask, right_mask, out_mask):
    rows = left_blocks.shape[0]
    depth, cols = right_blocks.shape
    share = rows // kk_n
    peers = kk_n // 2
    half = peers * share
    dma = pltpu.SemaphoreType.DMA
    f32, bf16 = jnp.float32, jnp.bfloat16
    return pl.pallas_call(
        functools.partial(kernel, rows_n, kk_n),
        out_shape=pltpu.VMEM((share, rows_n * cols), bf16),
        in_specs=[pl.BlockSpec(memory_space=pl.ANY)] * 2 + [pl.BlockSpec(memory_space=pltpu.SMEM)] * 3,
        out_specs=pl.BlockSpec(memory_space=pltpu.VMEM),
        scratch_shapes=[
            pltpu.VMEM((rows, depth), bf16),
            pltpu.VMEM((depth, cols), bf16),
            pltpu.VMEM((rows, depth), bf16),
            pltpu.VMEM((rows_n, depth, cols), bf16),
            pltpu.VMEM((rows_n, half, cols), f32),
            pltpu.VMEM((rows_n, half, cols), f32),
            pltpu.VMEM((rows_n, peers, share, cols), f32),
            pltpu.VMEM((rows_n, max(peers - 1, 1), share, cols), f32),
            dma((2,)),
            dma((rows_n, PIECES)),
            dma((rows_n + 1, PIECES)),
            dma((rows_n, PIECES)),
            dma((rows_n,)),
            dma((rows_n,)),
            dma((rows_n, max(peers - 1, 1))),
            dma((rows_n, max(peers - 1, 1))),
        ],
        compiler_params=pltpu.CompilerParams(
            collective_id=0, has_side_effects=True, vmem_limit_bytes=VMEM_BYTES - share * rows_n * cols * 2 - SPARE
        ),
    )(left_blocks, right_blocks, left_mask, right_mask.reshape(-1), out_mask)


def solution(mesh):
    in_specs = (P("row", "kk"), P("kk", "row"), P("row", "kk"), P("kk", "row"), P("row", None))
    out_specs = P(("row", "kk"), None)
    body = functools.partial(per_device, mesh.shape["row"], mesh.shape["kk"])
    return jax.shard_map(body, mesh=mesh, in_specs=in_specs, out_specs=out_specs, check_vma=False)
```
